32 devices in a mesh: wa: 16 (over z, y, core), ha: 2 (over x).
Axes of the slice: x: 2, y: 2, z: 4, core: 2. Of those that a mesh axis runs over, the one named last changes fastest.
Arguments:
- tokens: bfloat16 [16384, 4096], P('wa'), may hold values from -6 to 6
- expert_ids: int32 [16384, 8], P('wa'), may hold values from 0 to 127, as said below
- keep_mask: int32 [16384, 8], P('wa'), may hold values from 0 to 1, as said below
- route_weight: float32 [16384, 8], P('wa'), may hold values from 0.2 to 1
- gate_weight: bfloat16 [4096, 1536], P('wa', 'ha'), may hold values from -0.09375 to 0.09375
- up_weight: bfloat16 [4096, 1536], P('wa', 'ha'), may hold values from -0.09375 to 0.09375
- down_weight: bfloat16 [4096, 1536], P('wa', 'ha'), may hold values from -0.15625 to 0.15625
Outputs:
- mixed: bfloat16 [16384, 4096], P('wa', 'ha')
The draws below stay inside these ranges and needn't reach their ends.
Inputs may be any that keep to these rules, and one draw needn't show every extreme that they name: `expert_ids`: each row names 8 different experts. keep_mask[t, k] is 1 exactly where fewer than 128 earlier tokens of the same block of 1024 rows name expert_ids[t, k]; in some block 128 tokens naming expert 0 are kept.
All inputs are finite; a program needn't handle non-finite values.
Results may differ from the reference program's by a relative error of at most 0.005.
Values may be sent and summed in bfloat16 or wider, within the bound.
A program may use at most 128 MiB of HBM per device.

```python
import math
import jax
import jax.numpy as jnp
from jax import lax

D = 4096
HID = 1536
EXPERTS = 128
TOP = 8
TOK_DEV = 1024
CAP = 128
TOKENS = 16384
GLOBAL_CAP = 1024


def routing(key):
    block_count = TOKENS // TOK_DEV
    keys = jax.random.split(jax.random.fold_in(key, 11), 4)
    columns = jnp.arange(EXPERTS, dtype=jnp.int32)
    scores = jax.random.randint(keys[0], (TOKENS, EXPERTS), 0, 65536, dtype=jnp.int32) * EXPERTS + columns[None, :]
    boost_rate = jax.random.randint(keys[1], (block_count,), 1, 9, dtype=jnp.int32)
    forced = jax.random.randint(keys[2], (), 0, block_count, dtype=jnp.int32)
    boost_rate = jnp.where(jnp.arange(block_count, dtype=jnp.int32) == forced, 32, boost_rate)
    coin_flip = jax.random.randint(keys[3], (TOKENS,), 0, 32, dtype=jnp.int32)
    favoured = (coin_flip < jnp.repeat(boost_rate, TOK_DEV)).astype(jnp.int32)
    scores = scores.at[:, 0].add(favoured * 16777216)
    chosen_ids = lax.top_k(scores, TOP)[1].astype(jnp.int32)
    counts = jnp.zeros((TOKENS, EXPERTS), jnp.int32)
    for column in range(TOP):
        counts = counts + (chosen_ids[:, column:column + 1] == columns[None, :]).astype(jnp.int32)
    blocked = counts.reshape(block_count, TOK_DEV, EXPERTS)
    earlier = (jnp.cumsum(blocked, axis=1).astype(jnp.int32) - blocked).reshape(TOKENS, EXPERTS)
    position = jnp.take_along_axis(earlier, chosen_ids, axis=1)
    keeping = (position < CAP).astype(jnp.int32)
    return (chosen_ids, keeping)


def draw_expert_ids(key, part):
    return routing(key)[0]


def draw_keep_mask(key, part):
    return routing(key)[1]


def block_levels(own_key, dims, cuts, low, top_value):
    level, own = 1.0, jax.random.fold_in(own_key, 6)
    for axis_at, blocks in cuts:
        heights = jnp.exp(jax.random.uniform(jax.random.fold_in(own, axis_at), (blocks,), jnp.float32, low / len(cuts), top_value / len(cuts)))
        level = level * jnp.repeat(heights, dims[axis_at] // blocks).reshape([-1 if axis == axis_at else 1 for axis in range(len(dims))])
    return level


def normal_values(own_key, dims, spread, limit, cuts=(), kind=jnp.bfloat16):
    drawn = jax.random.normal(own_key, dims, jnp.float32) * spread
    if len(cuts) > 0:
        drawn = block_levels(own_key, dims, cuts, -0.22, 0.18) * drawn
    return jnp.clip(drawn, min=-limit, max=limit).astype(kind)


def setup_inputs(seed: int = 0) -> dict:
    splits = jax.random.split(jax.random.key(seed), 8)
    tokens = normal_values(splits[0], (TOKENS, D), 1.0, 6.0, ((0, 16),))
    expert_ids = draw_expert_ids(jax.random.fold_in(splits[7], 71), 0)
    keep_mask = draw_keep_mask(jax.random.fold_in(splits[7], 71), 0)
    route_weight = jnp.clip(jnp.exp(math.log(1.0) - 1.609438 * jax.random.uniform(splits[3], (TOKENS, TOP), jnp.float32) ** block_levels(splits[3], (TOKENS, TOP), ((0, 16),), -0.2, 0.2)), 0.2, 1.0)
    gate_weight = normal_values(splits[4], (D, HID), D ** -0.5, 0.09375, ((0, 16), (1, 2)))
    up_weight = normal_values(splits[5], (D, HID), D ** -0.5, 0.09375, ((0, 16), (1, 2)))
    down_weight = normal_values(splits[6], (D, HID), HID ** -0.5, 0.15625, ((0, 16), (1, 2)))
    return dict(tokens=tokens, expert_ids=expert_ids, keep_mask=keep_mask, route_weight=route_weight, gate_weight=gate_weight, up_weight=up_weight, down_weight=down_weight)


def reference(tokens, expert_ids, keep_mask, route_weight, gate_weight, up_weight, down_weight):
    block_count = TOKENS // TOK_DEV
    matches = (expert_ids == 0) & (keep_mask == 1)
    chosen = jnp.any(matches, axis=1).astype(jnp.int32).reshape(block_count, TOK_DEV)
    route_sum = jnp.sum(jnp.where(matches, route_weight, jnp.float32(0.0)), axis=1).astype(jnp.float32)
    route_sum = route_sum.reshape(block_count, TOK_DEV)
    position = (jnp.cumsum(chosen, axis=1).astype(jnp.int32) - chosen).astype(jnp.int32)
    counted = jnp.sum(chosen, axis=1).astype(jnp.int32)
    earlier = (jnp.cumsum(counted).astype(jnp.int32) - counted).astype(jnp.int32)
    admitted = chosen * ((earlier[:, None] + position) < GLOBAL_CAP).astype(jnp.int32)
    slot_ids = jnp.arange(CAP, dtype=jnp.int32)

    def one_block(packed):
        block_rows, block_pos, block_adm, block_route = packed
        dispatch = (block_pos[None, :] == slot_ids[:, None]) & (block_adm[None, :] == 1)
        slot_rows = jnp.dot(dispatch.astype(jnp.bfloat16), block_rows, preferred_element_type=jnp.float32).astype(jnp.bfloat16)
        gate_sum = jnp.dot(slot_rows, gate_weight, preferred_element_type=jnp.float32)
        up_sum = jnp.dot(slot_rows, up_weight, preferred_element_type=jnp.float32)
        hidden = (jax.nn.silu(gate_sum) * up_sum).astype(jnp.bfloat16)
        expert_out = jnp.dot(hidden, down_weight.T, preferred_element_type=jnp.float32)
        combine_map = jnp.where(dispatch.T, block_route[:, None], jnp.float32(0.0)).astype(jnp.float32)
        mixed_block = jnp.dot(combine_map, expert_out, precision=lax.Precision.HIGHEST, preferred_element_type=jnp.float32)
        return mixed_block.astype(jnp.bfloat16)

    mixed = lax.map(one_block, (tokens.reshape(block_count, TOK_DEV, D), position, admitted, route_sum))
    return mixed.reshape(TOKENS, D)
```

```python
import functools

import jax
import jax.numpy as jnp
from jax import lax
from jax.experimental import pallas as pl
from jax.experimental.pallas import tpu as pltpu
from jax.sharding import PartitionSpec as P

CAP = 128
TOK_COLS = 512
K_BLOCK = 1024
MESH = pl.DeviceIdType.MESH


def expert_kernel(
    n,
    pos_ref, count_ref, tok_ref, gate_ref, up_ref, down_ref,
    y_ref, earlier_ref,
    w, counts, slots, tok_buf, gate_acc, up_acc, hidden, own, sent, got,
    load_sem, tok_sem, c_send, c_recv, r_send, r_recv, d_send, d_recv, o_send, o_recv, x_send, x_recv,
):
    chips = n // 2
    half_ring = chips // 2
    cols = n // 2
    me = lax.axis_index("wa")
    ha = lax.axis_index("ha")
    core = lax.rem(me, 2)
    chip = me // 2
    odd = lax.rem(chip, 2)
    place = (1 - odd) * (chip // 2) + odd * (chips - 1 - chip // 2)

    def at(p):
        p = lax.rem(p + 2 * chips, chips)
        back = p // half_ring
        return 2 * ((1 - back) * 2 * p + back * (2 * (chips - 1 - p) + 1)) + core

    nxt, prv = at(place + 1), at(place - 1)
    sibling = me + 1 - 2 * core

    def origin(direction, step):
        return at(place - step) if direction == 0 else at(place + step)

    def piece(index, k):
        return w.at[k // 2, index, k % 2]

    def ring_send(direction, step, k):
        ref = piece(origin(direction, step - 1), k)
        return pltpu.make_async_remote_copy(
            src_ref=ref, dst_ref=ref,
            send_sem=r_send.at[direction, step - 1, k], recv_sem=r_recv.at[direction, step - 1, k],
            device_id={"wa": nxt if direction == 0 else prv}, device_id_type=MESH,
        )

    def ring_recv(direction, step, k):
        ref = piece(origin(direction, step), k)
        return pltpu.make_async_remote_copy(
            src_ref=ref, dst_ref=ref,
            send_sem=r_send.at[direction, step - 1, k], recv_sem=r_recv.at[direction, step - 1, k],
            device_id={"wa": nxt if direction == 0 else prv}, device_id_type=MESH,
        )

    def pass_on(direction, step, k):
        ref = piece(origin(direction, step), k)
        return pltpu.make_async_remote_copy(
            src_ref=ref, dst_ref=ref,
            send_sem=d_send.at[direction, step - 1, k], recv_sem=d_recv.at[direction, step - 1, k],
            device_id={"wa": sibling}, device_id_type=MESH,
        )

    def other(index):
        return index + 1 - 2 * core

    def passed(direction, step, k):
        ref = piece(other(origin(direction, step)), k)
        return pltpu.make_async_remote_copy(
            src_ref=ref, dst_ref=ref,
            send_sem=d_send.at[direction, step - 1, k], recv_sem=d_recv.at[direction, step - 1, k],
            device_id={"wa": sibling}, device_id_type=MESH,
        )

    def own_pass(t, index):
        return pltpu.make_async_remote_copy(
            src_ref=w.at[t, index], dst_ref=w.at[t, index],
            send_sem=o_send.at[t], recv_sem=o_recv.at[t],
            device_id={"wa": sibling}, device_id_type=MESH,
        )

    def count_copy(k):
        return pltpu.make_async_remote_copy(
            src_ref=count_ref, dst_ref=counts.at[me],
            send_sem=c_send.at[k], recv_sem=c_recv.at[k],
            device_id={"wa": lax.rem(me + k, n)}, device_id_type=MESH,
        )

    def count_got(k):
        return pltpu.make_async_remote_copy(
            src_ref=count_ref, dst_ref=counts.at[lax.rem(me - k + n, n)],
            send_sem=c_send.at[k], recv_sem=c_recv.at[k],
            device_id={"wa": lax.rem(me + k, n)}, device_id_type=MESH,
        )

    def swap(j):
        return pltpu.make_async_remote_copy(
            src_ref=sent.at[j], dst_ref=got.at[j],
            send_sem=x_send.at[j], recv_sem=x_recv.at[j],
            device_id={"ha": 1 - ha}, device_id_type=MESH,
        )

    loads = [
        pltpu.make_async_copy(ref, w.at[t, me], load_sem.at[t])
        for t, ref in enumerate((gate_ref, up_ref, down_ref))
    ]
    for load in loads:
        load.start()
    blocks = tok_ref.shape[1] // TOK_COLS

    def tok_load(i, slot):
        return pltpu.make_async_copy(
            tok_ref.at[:, pl.ds(pl.multiple_of(i * TOK_COLS, TOK_COLS), TOK_COLS)],
            tok_buf.at[slot], tok_sem.at[slot],
        )

    tok_load(0, 0).start()
    tok_load(1, 1).start()

    barrier = pltpu.get_barrier_semaphore()

    @pl.loop(1, n)
    def _(k):
        pl.semaphore_signal(barrier, inc=1, device_id={"wa": lax.rem(me + k, n)}, device_id_type=MESH)

    pl.semaphore_signal(barrier, inc=1, device_id={"ha": 1 - ha}, device_id_type=MESH)
    pl.semaphore_wait(barrier, n)

    for t in range(2):
        loads[t].wait()
        for k in (2 * t, 2 * t + 1):
            for direction in (0, 1):
                ring_send(direction, 1, k).start()
        own_pass(t, me).start()
    loads[2].wait()
    own_pass(2, me).start()

    @pl.loop(1, n)
    def _(k):
        count_copy(k).start()

    slot_ids = lax.broadcasted_iota(jnp.int32, (CAP, pos_ref.shape[1]), 0)
    table = jnp.where(pos_ref[...] == slot_ids, jnp.float32(1.0), jnp.float32(0.0)).astype(jnp.bfloat16)

    @pl.loop(0, blocks)
    def _(i):
        slot = lax.rem(i, 2)
        tok_load(i, slot).wait()
        slots[:, pl.ds(pl.multiple_of(i * TOK_COLS, TOK_COLS), TOK_COLS)] = jnp.dot(
            table, tok_buf[slot], preferred_element_type=jnp.float32
        ).astype(jnp.bfloat16)

        @pl.when(i + 2 < blocks)
        def _():
            tok_load(i + 2, slot).start()

    def serve(step, streams, last_forward):
        for k in streams:
            for direction in (0, 1):
                ring_recv(direction, step, k).wait_recv()
                if not last_forward or k % 2 == direction:
                    ring_send(direction, step + 1, k).start()
                pass_on(direction, step, k).start()

    def serve_end(streams):
        for k in streams:
            direction = k % 2
            ring_recv(direction, half_ring, k).wait_recv()
            pass_on(direction, half_ring, k).start()

    early, late = (0, 1, 2, 3), (4, 5)

    @pl.loop(1, half_ring - 1)
    def _(step):
        serve(step, early, False)

    serve(half_ring - 1, early, True)
    for k in late:
        for direction in (0, 1):
            ring_send(direction, 1, k).start()
    serve_end(early)

    for t in (0, 1):
        own_pass(t, sibling).wait_recv()

    @pl.loop(1, half_ring)
    def _(step):
        for k in early:
            for direction in (0, 1):
                passed(direction, step, k).wait_recv()

    for k in early:
        passed(k % 2, half_ring, k).wait_recv()

    fd = w.shape[2] * w.shape[3]
    per = K_BLOCK // fd
    hid = w.shape[4]
    gate_acc[...] = jnp.zeros_like(gate_acc)
    up_acc[...] = jnp.zeros_like(up_acc)

    @pl.loop(0, n // per)
    def _(i):
        rows = slots[:, pl.ds(pl.multiple_of(i * K_BLOCK, K_BLOCK), K_BLOCK)]
        for t, acc in ((0, gate_acc), (1, up_acc)):
            block = w[t, pl.ds(i * per, per)].reshape(K_BLOCK, hid)
            acc[...] += jnp.dot(rows, block, preferred_element_type=jnp.float32)

    gate = gate_acc[...]
    hidden[...] = (gate / (1.0 + jnp.exp(-gate)) * up_acc[...]).astype(jnp.bfloat16)

    def finish(index):
        part = lax.dot_general(
            hidden[...], w[2, index].reshape(fd, hid), (((1,), (1,)), ((), ())),
            preferred_element_type=jnp.float32,
        )
        j = lax.rem(index, cols)

        @pl.when(index // cols == ha)
        def _():
            own[j] = part

        @pl.when(index // cols != ha)
        def _():
            sent[j] = part.astype(jnp.bfloat16)
            swap(j).start()

    finish(me)
    own_pass(2, sibling).wait_recv()
    finish(sibling)

    def down_step(step):
        for direction in (0, 1):
            index = origin(direction, step)
            finish(index)
            for k in late:
                passed(direction, step, k).wait_recv()
            finish(other(index))

    @pl.loop(1, half_ring - 1)
    def _(step):
        serve(step, late, False)
        down_step(step)

    serve(half_ring - 1, late, True)
    down_step(half_ring - 1)
    serve_end(late)
    far = origin(0, half_ring)
    finish(far)
    for k in late:
        passed(k % 2, half_ring, k).wait_recv()
    finish(other(far))

    @pl.loop(1, n)
    def _(k):
        count_got(k).wait_recv()

    counts[me] = jnp.zeros(counts.shape[1:], jnp.int32)
    total = jnp.zeros(counts.shape[1:], jnp.int32)

    def add_count(i, total):
        return total + jnp.where(i < me, counts[i], 0)

    earlier_ref[...] = lax.fori_loop(0, n, add_count, total)

    for j in range(cols):
        swap(j).wait_recv()
        y = own[j] + got[j].astype(jnp.float32)
        high = y.astype(jnp.bfloat16)
        y_ref[0:CAP, j * fd:(j + 1) * fd] = high
        y_ref[CAP:2 * CAP, j * fd:(j + 1) * fd] = (y - high.astype(jnp.float32)).astype(jnp.bfloat16)

    @pl.loop(1, n)
    def _(k):
        count_copy(k).wait_send()

    for t in range(3):
        own_pass(t, me).wait_send()

    @pl.loop(1, half_ring)
    def _(step):
        for k in range(6):
            for direction in (0, 1):
                ring_send(direction, step, k).wait_send()
                pass_on(direction, step, k).wait_send()

    for k in range(6):
        ring_send(k % 2, half_ring, k).wait_send()
        pass_on(k % 2, half_ring, k).wait_send()

    @pl.loop(0, cols)
    def _(j):
        swap(j).wait_send()


def expert(pos, count, tokens, gate, up, down):
    n = lax.axis_size("wa")
    fd, hid = gate.shape
    half = fd // 2
    steps = n // 4
    cols = n // 2
    any_spec = pl.BlockSpec(memory_space=pl.ANY)
    vmem = pl.BlockSpec(memory_space=pltpu.VMEM)
    dma = pltpu.SemaphoreType.DMA
    return pl.pallas_call(
        functools.partial(expert_kernel, n),
        out_shape=(
            jax.ShapeDtypeStruct((2 * CAP, cols * fd), jnp.bfloat16),
            jax.ShapeDtypeStruct(count.shape, jnp.int32),
        ),
        in_specs=[vmem, vmem, any_spec, any_spec, any_spec, any_spec],
        out_specs=(vmem, vmem),
        scratch_shapes=[
            pltpu.VMEM((3, n, 2, half, hid), jnp.bfloat16),
            pltpu.VMEM((n, *count.shape), jnp.int32),
            pltpu.VMEM((CAP, n * fd), jnp.bfloat16),
            pltpu.VMEM((2, tokens.shape[0], TOK_COLS), jnp.bfloat16),
            pltpu.VMEM((CAP, hid), jnp.float32),
            pltpu.VMEM((CAP, hid), jnp.float32),
            pltpu.VMEM((CAP, hid), jnp.bfloat16),
            pltpu.VMEM((cols, CAP, fd), jnp.float32),
            pltpu.VMEM((cols, CAP, fd), jnp.bfloat16),
            pltpu.VMEM((cols, CAP, fd), jnp.bfloat16),
            dma((3,)), dma((2,)), dma((n,)), dma((n,)),
            dma((2, steps, 6)), dma((2, steps, 6)),
            dma((2, steps, 6)), dma((2, steps, 6)),
            dma((3,)), dma((3,)), dma((cols,)), dma((cols,)),
        ],
        compiler_params=pltpu.CompilerParams(
            collective_id=0, has_side_effects=True, vmem_limit_bytes=60 * 1024 * 1024
        ),
    )(pos, count, tokens, *(v.reshape(2, half, hid) for v in (gate, up, down)))


def per_device(tokens, expert_ids, keep_mask, route_weight, gate_weight, up_weight, down_weight):
    matches = (expert_ids == 0) & (keep_mask == 1)
    chosen = jnp.any(matches, axis=1).astype(jnp.int32)
    route_sum = jnp.sum(jnp.where(matches, route_weight, jnp.float32(0.0)), axis=1)
    position = jnp.cumsum(chosen) - chosen
    place = jnp.where(chosen == 1, position, -1)
    count = jnp.broadcast_to(jnp.sum(chosen), (8, 128))
    y, earlier = expert(place[None, :], count, tokens, gate_weight, up_weight, down_weight)
    capacity = lax.axis_size("wa") * CAP // 2
    slot_ids = lax.rem(jnp.arange(2 * CAP, dtype=jnp.int32), CAP)
    admitted = (place[:, None] == slot_ids[None, :]) & (earlier[0, 0] + place < capacity)[:, None]
    mixed = jnp.dot(admitted.astype(jnp.bfloat16), y, preferred_element_type=jnp.float32)
    return (mixed * route_sum[:, None]).astype(jnp.bfloat16)


def solution(mesh):
    return jax.shard_map(
        per_device,
        mesh=mesh,
        in_specs=(
            P("wa", None),
            P("wa", None),
            P("wa", None),
            P("wa", None),
            P("wa", "ha"),
            P("wa", "ha"),
            P("wa", "ha"),
        ),
        out_specs=P("wa", "ha"),
        check_vma=False,
    )
```

```python
import functools

import jax
import jax.numpy as jnp
from jax import lax
from jax.experimental import pallas as pl
from jax.experimental.pallas import tpu as pltpu
from jax.sharding import PartitionSpec as P

CAP = 128
TOK_COLS = 512
MESH = pl.DeviceIdType.MESH


def expert_kernel(
    n,
    pos_ref, tok_ref, gate_ref, up_ref, down_ref,
    y_ref,
    w, wd, count, counts, slots, guest, tok_buf, part_out, part_in, gate_acc, up_acc, hidden, own, sent, got,
    load_sem, tok_sem, c_send, c_recv, r_send, r_recv, d_send, d_recv, rd_send, rd_recv, dd_send, dd_recv,
    o_send, o_recv, g_send, g_recv, h_send, h_recv, p_send, p_recv, x_send, x_recv,
):
    side = n // 2
    me = lax.axis_index("wa")
    ha = lax.axis_index("ha")
    core = lax.rem(me, 2)
    half = me // side
    sibling = me + 1 - 2 * core
    across = lax.rem(me + side, n)

    def remote(ref, dst, send, recv, **where):
        return pltpu.make_async_remote_copy(
            src_ref=ref, dst_ref=dst, send_sem=send, recv_sem=recv, device_id=where, device_id_type=MESH
        )

    class Ring:
        def __init__(self, members, base, ref_of, sems):
            self.chips, self.base, self.ref_of = members // 2, base, ref_of
            self.steps = self.chips // 2
            self.r_send, self.r_recv, self.d_send, self.d_recv = sems
            chip = (me - base) // 2
            odd = lax.rem(chip, 2)
            self.place = (1 - odd) * (chip // 2) + odd * (self.chips - 1 - chip // 2)
            self.to = (base + self.at(self.place + 1), base + self.at(self.place - 1))

        def at(self, p):
            p = lax.rem(p + 2 * self.chips, self.chips)
            back = p // self.steps
            return 2 * ((1 - back) * 2 * p + back * (2 * (self.chips - 1 - p) + 1)) + core

        def origin(self, direction, step):
            return self.at(self.place - step) if direction == 0 else self.at(self.place + step)

        def _hop(self, ref, direction, step, k):
            return remote(
                ref, ref, self.r_send.at[direction, step - 1, k], self.r_recv.at[direction, step - 1, k],
                wa=self.to[direction],
            )

        def _pass(self, ref, direction, step, k):
            return remote(
                ref, ref, self.d_send.at[direction, step - 1, k], self.d_recv.at[direction, step - 1, k], wa=sibling
            )

        def send(self, direction, step, k):
            return self._hop(self.ref_of(self.origin(direction, step - 1), k), direction, step, k)

        def recv(self, direction, step, k):
            return self._hop(self.ref_of(self.origin(direction, step), k), direction, step, k)

        def pass_on(self, direction, step, k):
            return self._pass(self.ref_of(self.origin(direction, step), k), direction, step, k)

        def passed(self, direction, step, k):
            index = self.origin(direction, step) + 1 - 2 * core
            return self._pass(self.ref_of(index, k), direction, step, k)

        def serve(self, step, streams, last_forward):
            for k in streams:
                for direction in (0, 1):
                    self.recv(direction, step, k).wait_recv()
                    if not last_forward or k % 2 == direction:
                        self.send(direction, step + 1, k).start()
                    self.pass_on(direction, step, k).start()

        def serve_end(self, streams):
            for k in streams:
                self.recv(k % 2, self.steps, k).wait_recv()
                self.pass_on(k % 2, self.steps, k).start()

        def drain(self, streams):
            @pl.loop(1, self.steps)
            def _(step):
                for k in streams:
                    for direction in (0, 1):
                        self.send(direction, step, k).wait_send()
                        self.pass_on(direction, step, k).wait_send()

            for k in streams:
                self.send(k % 2, self.steps, k).wait_send()
                self.pass_on(k % 2, self.steps, k).wait_send()

    near = Ring(side, half * side, lambda i, k: w.at[k // 2, i, k % 2], (r_send, r_recv, d_send, d_recv))
    full = Ring(n, 0, lambda i, k: wd.at[i, k], (rd_send, rd_recv, dd_send, dd_recv))
    mine = me - half * side
    early, late = (0, 1, 2, 3), (0, 1)

    def own_pass(t, index):
        ref = wd.at[index] if t == 2 else w.at[t, index - half * side]
        return remote(ref, ref, o_send.at[t], o_recv.at[t], wa=sibling)

    def count_copy(k):
        return remote(count, counts.at[me], c_send.at[k], c_recv.at[k], wa=lax.rem(me + k, n))

    def count_got(k):
        return remote(count, counts.at[lax.rem(me - k + n, n)], c_send.at[k], c_recv.at[k], wa=lax.rem(me + k, n))

    def swap(j):
        return remote(sent.at[j], got.at[j], x_send.at[j], x_recv.at[j], ha=1 - ha)

    loads = [
        pltpu.make_async_copy(gate_ref, w.at[0, mine], load_sem.at[0]),
        pltpu.make_async_copy(up_ref, w.at[1, mine], load_sem.at[1]),
        pltpu.make_async_copy(down_ref, wd.at[me], load_sem.at[2]),
    ]
    for load in loads:
        load.start()
    quarter = slots.shape[2]
    per_quarter = quarter // TOK_COLS
    leaving = 2 * (1 - half) + ha
    wanted = (leaving, 2 * half, 2 * half + 1)
    blocks = len(wanted) * per_quarter

    def tok_load(i):
        start = wanted[i // per_quarter] * quarter + i % per_quarter * TOK_COLS
        return pltpu.make_async_copy(
            tok_ref.at[:, pl.ds(pl.multiple_of(start, TOK_COLS), TOK_COLS)], tok_buf.at[i % 2], tok_sem.at[i % 2]
        )

    tok_load(0).start()
    tok_load(1).start()
    place = pos_ref[...]
    chosen = jnp.sum(jnp.where(place >= 0, 1, 0), axis=1, keepdims=True)
    count[...] = jnp.broadcast_to(chosen, count.shape)

    barrier = pltpu.get_barrier_semaphore()

    @pl.loop(1, n)
    def _(k):
        pl.semaphore_signal(barrier, inc=1, device_id={"wa": lax.rem(me + k, n)}, device_id_type=MESH)

    pl.semaphore_signal(barrier, inc=1, device_id={"ha": 1 - ha}, device_id_type=MESH)
    pl.semaphore_wait(barrier, n)

    for t in range(2):
        loads[t].wait()
        for k in (2 * t, 2 * t + 1):
            for direction in (0, 1):
                near.send(direction, 1, k).start()
        own_pass(t, me).start()
    loads[2].wait()
    own_pass(2, me).start()

    slot_ids = lax.broadcasted_iota(jnp.int32, (CAP, pos_ref.shape[1]), 0)
    table = jnp.where(place == slot_ids, jnp.float32(1.0), jnp.float32(0.0)).astype(jnp.bfloat16)
    guest_out = remote(slots.at[0], guest.at[ha], g_send, g_recv, wa=across)
    guest_in = guest_out
    share = remote(guest.at[ha], guest.at[ha], h_send, h_recv, ha=1 - ha)
    shared = remote(guest.at[1 - ha], guest.at[1 - ha], h_send, h_recv, ha=1 - ha)
    for i in range(blocks):
        tok_load(i).wait()
        slots[i // per_quarter, :, i % per_quarter * TOK_COLS:(i % per_quarter + 1) * TOK_COLS] = jnp.dot(
            table, tok_buf[i % 2], preferred_element_type=jnp.float32
        ).astype(jnp.bfloat16)
        if i + 2 < blocks:
            tok_load(i + 2).start()
        if i == per_quarter:
            guest_out.start()

    @pl.loop(1, n)
    def _(k):
        count_copy(k).start()

    @pl.loop(1, near.steps - 1)
    def _(step):
        near.serve(step, early, False)

    near.serve(near.steps - 1, early, True)
    guest_in.wait_recv()
    share.start()
    for k in late:
        for direction in (0, 1):
            full.send(direction, 1, k).start()
    near.serve_end(early)
    for t in (0, 1):
        own_pass(t, sibling).wait_recv()

    @pl.loop(1, near.steps)
    def _(step):
        for k in early:
            for direction in (0, 1):
                near.passed(direction, step, k).wait_recv()

    for k in early:
        near.passed(k % 2, near.steps, k).wait_recv()
    shared.wait_recv()

    hid = w.shape[4]
    group = side // 2

    def project(rows, t):
        total = None
        for q in (0, 1):
            block = w[t, q * group:(q + 1) * group].reshape(quarter, hid)
            term = jnp.dot(rows[q], block, preferred_element_type=jnp.float32)
            total = term if total is None else total + term
        return total

    def partial(t):
        return remote(part_out.at[t], part_in.at[t], p_send.at[t], p_recv.at[t], wa=across)

    part_out[0] = project((guest[0], guest[1]), 0).astype(jnp.bfloat16)
    part_out[1] = project((guest[0], guest[1]), 1).astype(jnp.bfloat16)
    partial(0).start()
    partial(1).start()
    gate_acc[...] = project((slots[1], slots[2]), 0)
    up_acc[...] = project((slots[1], slots[2]), 1)

    ahead = full.steps // 2

    @pl.loop(1, ahead + 1)
    def _(step):
        full.serve(step, late, False)

    partial(0).wait_recv()
    partial(1).wait_recv()
    gate = gate_acc[...] + part_in[0].astype(jnp.float32)
    up = up_acc[...] + part_in[1].astype(jnp.float32)
    hidden[...] = (gate / (1.0 + jnp.exp(-gate)) * up).astype(jnp.bfloat16)
    fd = wd.shape[1] * wd.shape[2]

    def finish(index):
        part = lax.dot_general(
            hidden[...], wd[index].reshape(fd, hid), (((1,), (1,)), ((), ())),
            preferred_element_type=jnp.float32,
        )
        j = lax.rem(index, side)

        @pl.when(index // side == ha)
        def _():
            own[j] = part

        @pl.when(index // side != ha)
        def _():
            sent[j] = part.astype(jnp.bfloat16)
            swap(j).start()

    finish(me)
    own_pass(2, sibling).wait_recv()
    finish(sibling)

    def down_step(step):
        for direction in (0, 1):
            index = full.origin(direction, step)
            finish(index)
            for k in late:
                full.passed(direction, step, k).wait_recv()
            finish(index + 1 - 2 * core)

    @pl.loop(1, ahead + 1)
    def _(step):
        down_step(step)

    @pl.loop(ahead + 1, full.steps - 1)
    def _(step):
        full.serve(step, late, False)
        down_step(step)

    full.serve(full.steps - 1, late, True)
    down_step(full.steps - 1)
    full.serve_end(late)
    far = full.origin(0, full.steps)
    finish(far)
    for k in late:
        full.passed(k % 2, full.steps, k).wait_recv()
    finish(far + 1 - 2 * core)

    @pl.loop(1, n)
    def _(k):
        count_got(k).wait_recv()

    counts[me] = jnp.zeros(counts.shape[1:], jnp.int32)

    def add_count(i, total):
        return total + jnp.where(i < me, counts[i], 0)

    earlier = lax.fori_loop(0, n, add_count, jnp.zeros(counts.shape[1:], jnp.int32))
    slot = lax.broadcasted_iota(jnp.int32, (CAP, fd), 0)
    admitted = slot + earlier[0:1, 0:1] < side * CAP

    for j in range(side):
        swap(j).wait_recv()
        y = jnp.where(admitted, own[j] + got[j].astype(jnp.float32), jnp.float32(0.0))
        high = y.astype(jnp.bfloat16)
        y_ref[0:CAP, j * fd:(j + 1) * fd] = high
        y_ref[CAP:2 * CAP, j * fd:(j + 1) * fd] = (y - high.astype(jnp.float32)).astype(jnp.bfloat16)

    @pl.loop(1, n)
    def _(k):
        count_copy(k).wait_send()

    for t in range(3):
        own_pass(t, me).wait_send()
    guest_out.wait_send()
    share.wait_send()
    partial(0).wait_send()
    partial(1).wait_send()
    near.drain(early)
    full.drain(late)

    @pl.loop(0, side)
    def _(j):
        swap(j).wait_send()


def expert(pos, tokens, gate, up, down):
    n = lax.axis_size("wa")
    fd, hid = gate.shape
    half = fd // 2
    side = n // 2
    quarter = tokens.shape[1] // 4
    any_spec = pl.BlockSpec(memory_space=pl.ANY)
    vmem = pl.BlockSpec(memory_space=pltpu.VMEM)
    dma = pltpu.SemaphoreType.DMA
    return pl.pallas_call(
        functools.partial(expert_kernel, n),
        out_shape=jax.ShapeDtypeStruct((2 * CAP, side * fd), jnp.bfloat16),
        in_specs=[vmem, any_spec, any_spec, any_spec, any_spec],
        out_specs=vmem,
        scratch_shapes=[
            pltpu.VMEM((2, side, 2, half, hid), jnp.bfloat16),
            pltpu.VMEM((n, 2, half, hid), jnp.bfloat16),
            pltpu.VMEM((8, 128), jnp.int32),
            pltpu.VMEM((n, 8, 128), jnp.int32),
            pltpu.VMEM((3, CAP, quarter), jnp.bfloat16),
            pltpu.VMEM((2, CAP, quarter), jnp.bfloat16),
            pltpu.VMEM((2, tokens.shape[0], TOK_COLS), jnp.bfloat16),
            pltpu.VMEM((2, CAP, hid), jnp.bfloat16),
            pltpu.VMEM((2, CAP, hid), jnp.bfloat16),
            pltpu.VMEM((CAP, hid), jnp.float32),
            pltpu.VMEM((CAP, hid), jnp.float32),
            pltpu.VMEM((CAP, hid), jnp.bfloat16),
            pltpu.VMEM((side, CAP, fd), jnp.float32),
            pltpu.VMEM((side, CAP, fd), jnp.bfloat16),
            pltpu.VMEM((side, CAP, fd), jnp.bfloat16),
            dma((3,)), dma((2,)), dma((n,)), dma((n,)),
            *[dma((2, n // 8, 4)) for _ in range(4)],
            *[dma((2, n // 4, 2)) for _ in range(4)],
            dma((3,)), dma((3,)), dma, dma, dma, dma, dma((2,)), dma((2,)), dma((side,)), dma((side,)),
        ],
        compiler_params=pltpu.CompilerParams(
            collective_id=0, has_side_effects=True, vmem_limit_bytes=60 * 1024 * 1024
        ),
    )(pos, tokens, *(v.reshape(2, half, hid) for v in (gate, up, down)))


def per_device(tokens, expert_ids, keep_mask, route_weight, gate_weight, up_weight, down_weight):
    matches = (expert_ids == 0) & (keep_mask == 1)
    chosen = jnp.any(matches, axis=1).astype(jnp.int32)
    route_sum = jnp.sum(jnp.where(matches, route_weight, jnp.float32(0.0)), axis=1)
    position = jnp.cumsum(chosen) - chosen
    place = jnp.where(chosen == 1, position, -1)
    y = expert(place[None, :], tokens, gate_weight, up_weight, down_weight)
    slot_ids = lax.rem(jnp.arange(2 * CAP, dtype=jnp.int32), CAP)
    combine = (place[:, None] == slot_ids[None, :]).astype(jnp.bfloat16)
    mixed = jnp.dot(combine, y, preferred_element_type=jnp.float32)
    return (mixed * route_sum[:, None]).astype(jnp.bfloat16)


def solution(mesh):
    return jax.shard_map(
        per_device,
        mesh=mesh,
        in_specs=(
            P("wa", None),
            P("wa", None),
            P("wa", None),
            P("wa", None),
            P("wa", "ha"),
            P("wa", "ha"),
            P("wa", "ha"),
        ),
        out_specs=P("wa", "ha"),
        check_vma=False,
    )
```

```python
import functools

import jax
import jax.numpy as jnp
from jax import lax
from jax.experimental import pallas as pl
from jax.experimental.pallas import tpu as pltpu
from jax.sharding import PartitionSpec as P

CAP = 128
TOK_COLS = 512
MESH = pl.DeviceIdType.MESH


def expert_kernel(
    n,
    pos_ref, tok_ref, gate_ref, up_ref, down_ref,
    y_ref,
    w, wd, count, counts, slots, guest, tok_buf, part_out, part_in, gate_acc, up_acc, hidden, own, sent, got,
    load_sem, tok_sem, c_send, c_recv, r_send, r_recv, d_send, d_recv, rd_send, rd_recv, dd_send, dd_recv,
    o_send, o_recv, g_send, g_recv, h_send, h_recv, p_send, p_recv, x_send, x_recv,
):
    side = n // 2
    me = lax.axis_index("wa")
    ha = lax.axis_index("ha")
    core = lax.rem(me, 2)
    half = me // side
    sibling = me + 1 - 2 * core
    across = lax.rem(me + side, n)

    def remote(ref, dst, send, recv, **where):
        return pltpu.make_async_remote_copy(
            src_ref=ref, dst_ref=dst, send_sem=send, recv_sem=recv, device_id=where, device_id_type=MESH
        )

    class Ring:
        def __init__(self, members, base, ref_of, sems):
            self.chips, self.base, self.ref_of = members // 2, base, ref_of
            self.steps = self.chips // 2
            self.r_send, self.r_recv, self.d_send, self.d_recv = sems
            chip = (me - base) // 2
            odd = lax.rem(chip, 2)
            self.place = (1 - odd) * (chip // 2) + odd * (self.chips - 1 - chip // 2)
            self.to = (base + self.at(self.place + 1), base + self.at(self.place - 1))

        def at(self, p):
            p = lax.rem(p + 2 * self.chips, self.chips)
            back = p // self.steps
            return 2 * ((1 - back) * 2 * p + back * (2 * (self.chips - 1 - p) + 1)) + core

        def origin(self, direction, step):
            return self.at(self.place - step) if direction == 0 else self.at(self.place + step)

        def _hop(self, ref, direction, step, k):
            return remote(
                ref, ref, self.r_send.at[direction, step - 1, k], self.r_recv.at[direction, step - 1, k],
                wa=self.to[direction],
            )

        def _pass(self, ref, direction, step, k):
            return remote(
                ref, ref, self.d_send.at[direction, step - 1, k], self.d_recv.at[direction, step - 1, k], wa=sibling
            )

        def send(self, direction, step, k):
            return self._hop(self.ref_of(self.origin(direction, step - 1), k), direction, step, k)

        def recv(self, direction, step, k):
            return self._hop(self.ref_of(self.origin(direction, step), k), direction, step, k)

        def pass_on(self, direction, step, k):
            return self._pass(self.ref_of(self.origin(direction, step), k), direction, step, k)

        def passed(self, direction, step, k):
            index = self.origin(direction, step) + 1 - 2 * core
            return self._pass(self.ref_of(index, k), direction, step, k)

        def serve(self, step, streams, last_forward):
            for k in streams:
                for direction in (0, 1):
                    self.recv(direction, step, k).wait_recv()
                    if not last_forward or k % 2 == direction:
                        self.send(direction, step + 1, k).start()
                    self.pass_on(direction, step, k).start()

        def serve_end(self, streams):
            for k in streams:
                self.recv(k % 2, self.steps, k).wait_recv()
                self.pass_on(k % 2, self.steps, k).start()

        def drain(self, streams):
            @pl.loop(1, self.steps)
            def _(step):
                for k in streams:
                    for direction in (0, 1):
                        self.send(direction, step, k).wait_send()
                        self.pass_on(direction, step, k).wait_send()

            for k in streams:
                self.send(k % 2, self.steps, k).wait_send()
                self.pass_on(k % 2, self.steps, k).wait_send()

    near = Ring(side, half * side, lambda i, k: w.at[k // 2, i, k % 2], (r_send, r_recv, d_send, d_recv))
    full = Ring(n, 0, lambda i, k: wd.at[i, k], (rd_send, rd_recv, dd_send, dd_recv))
    mine = me - half * side
    early, late = (0, 1, 2, 3), (0, 1)

    def own_pass(t, index):
        ref = wd.at[index] if t == 2 else w.at[t, index - half * side]
        return remote(ref, ref, o_send.at[t], o_recv.at[t], wa=sibling)

    def count_copy(k):
        return remote(count, counts.at[me], c_send.at[k], c_recv.at[k], wa=lax.rem(me + k, n))

    def count_got(k):
        return remote(count, counts.at[lax.rem(me - k + n, n)], c_send.at[k], c_recv.at[k], wa=lax.rem(me + k, n))

    def swap(j):
        return remote(sent.at[j], got.at[j], x_send.at[j], x_recv.at[j], ha=1 - ha)

    loads = [
        pltpu.make_async_copy(gate_ref, w.at[0, mine], load_sem.at[0]),
        pltpu.make_async_copy(up_ref, w.at[1, mine], load_sem.at[1]),
        pltpu.make_async_copy(down_ref, wd.at[me], load_sem.at[2]),
    ]
    for load in loads:
        load.start()
    quarter = slots.shape[2]
    per_quarter = quarter // TOK_COLS
    leaving = 2 * (1 - half) + ha
    wanted = (leaving, 2 * half, 2 * half + 1)
    blocks = len(wanted) * per_quarter

    def tok_load(i):
        start = wanted[i // per_quarter] * quarter + i % per_quarter * TOK_COLS
        return pltpu.make_async_copy(
            tok_ref.at[:, pl.ds(pl.multiple_of(start, TOK_COLS), TOK_COLS)], tok_buf.at[i % 2], tok_sem.at[i % 2]
        )

    tok_load(0).start()
    tok_load(1).start()
    place = pos_ref[...]
    chosen = jnp.sum(jnp.where(place >= 0, 1, 0), axis=1, keepdims=True)
    count[...] = jnp.broadcast_to(chosen, count.shape)

    barrier = pltpu.get_barrier_semaphore()

    @pl.loop(1, n)
    def _(k):
        pl.semaphore_signal(barrier, inc=1, device_id={"wa": lax.rem(me + k, n)}, device_id_type=MESH)

    pl.semaphore_signal(barrier, inc=1, device_id={"ha": 1 - ha}, device_id_type=MESH)
    pl.semaphore_wait(barrier, n)

    for t in range(2):
        loads[t].wait()
        for k in (2 * t, 2 * t + 1):
            for direction in (0, 1):
                near.send(direction, 1, k).start()
        own_pass(t, me).start()
    loads[2].wait()
    own_pass(2, me).start()

    slot_ids = lax.broadcasted_iota(jnp.int32, (CAP, pos_ref.shape[1]), 0)
    table = jnp.where(place == slot_ids, jnp.float32(1.0), jnp.float32(0.0)).astype(jnp.bfloat16)
    guest_out = remote(slots.at[0], guest.at[ha], g_send, g_recv, wa=across)
    guest_in = guest_out
    share = remote(guest.at[ha], guest.at[ha], h_send, h_recv, ha=1 - ha)
    shared = remote(guest.at[1 - ha], guest.at[1 - ha], h_send, h_recv, ha=1 - ha)
    for i in range(blocks):
        tok_load(i).wait()
        slots[i // per_quarter, :, i % per_quarter * TOK_COLS:(i % per_quarter + 1) * TOK_COLS] = jnp.dot(
            table, tok_buf[i % 2], preferred_element_type=jnp.float32
        ).astype(jnp.bfloat16)
        if i + 2 < blocks:
            tok_load(i + 2).start()
        if i == per_quarter:
            guest_out.start()

    @pl.loop(1, n)
    def _(k):
        count_copy(k).start()

    @pl.loop(1, near.steps - 1)
    def _(step):
        near.serve(step, early, False)

    near.serve(near.steps - 1, early, True)
    guest_in.wait_recv()
    share.start()
    for k in late:
        for direction in (0, 1):
            full.send(direction, 1, k).start()
    hid = w.shape[4]
    group = side // 2

    def project(rows, t):
        total = None
        for q in (0, 1):
            block = w[t, q * group:(q + 1) * group].reshape(quarter, hid)
            term = jnp.dot(rows[q], block, preferred_element_type=jnp.float32)
            total = term if total is None else total + term
        return total

    def partial(t):
        return remote(part_out.at[t], part_in.at[t], p_send.at[t], p_recv.at[t], wa=across)

    def gathered(t):
        streams = (2 * t, 2 * t + 1)
        near.serve_end(streams)
        own_pass(t, sibling).wait_recv()

        @pl.loop(1, near.steps)
        def _(step):
            for k in streams:
                for direction in (0, 1):
                    near.passed(direction, step, k).wait_recv()

        for k in streams:
            near.passed(k % 2, near.steps, k).wait_recv()

    gathered(0)
    shared.wait_recv()
    part_out[0] = project((guest[0], guest[1]), 0).astype(jnp.bfloat16)
    gate_acc[...] = project((slots[1], slots[2]), 0)
    partial(0).start()
    gathered(1)
    part_out[1] = project((guest[0], guest[1]), 1).astype(jnp.bfloat16)
    partial(1).start()
    up_acc[...] = project((slots[1], slots[2]), 1)

    @pl.loop(1, full.steps - 1)
    def _(step):
        full.serve(step, late, False)

    full.serve(full.steps - 1, late, True)
    partial(0).wait_recv()
    partial(1).wait_recv()
    gate = gate_acc[...] + part_in[0].astype(jnp.float32)
    up = up_acc[...] + part_in[1].astype(jnp.float32)
    hidden[...] = (gate / (1.0 + jnp.exp(-gate)) * up).astype(jnp.bfloat16)
    fd = wd.shape[1] * wd.shape[2]

    def finish(index):
        part = lax.dot_general(
            hidden[...], wd[index].reshape(fd, hid), (((1,), (1,)), ((), ())),
            preferred_element_type=jnp.float32,
        )
        j = lax.rem(index, side)

        @pl.when(index // side == ha)
        def _():
            own[j] = part

        @pl.when(index // side != ha)
        def _():
            sent[j] = part.astype(jnp.bfloat16)
            swap(j).start()

    finish(me)
    own_pass(2, sibling).wait_recv()
    finish(sibling)

    def down_step(step):
        for direction in (0, 1):
            index = full.origin(direction, step)
            finish(index)
            for k in late:
                full.passed(direction, step, k).wait_recv()
            finish(index + 1 - 2 * core)

    @pl.loop(1, full.steps - 1)
    def _(step):
        down_step(step)

    full.serve_end(late)
    down_step(full.steps - 1)
    far = full.origin(0, full.steps)
    finish(far)
    for k in late:
        full.passed(k % 2, full.steps, k).wait_recv()
    finish(far + 1 - 2 * core)

    @pl.loop(1, n)
    def _(k):
        count_got(k).wait_recv()

    counts[me] = jnp.zeros(counts.shape[1:], jnp.int32)

    def add_count(i, total):
        return total + jnp.where(i < me, counts[i], 0)

    earlier = lax.fori_loop(0, n, add_count, jnp.zeros(counts.shape[1:], jnp.int32))
    slot = lax.broadcasted_iota(jnp.int32, (CAP, fd), 0)
    admitted = slot + earlier[0:1, 0:1] < side * CAP

    for j in range(side):
        swap(j).wait_recv()
        y = jnp.where(admitted, own[j] + got[j].astype(jnp.float32), jnp.float32(0.0))
        high = y.astype(jnp.bfloat16)
        y_ref[0:CAP, j * fd:(j + 1) * fd] = high
        y_ref[CAP:2 * CAP, j * fd:(j + 1) * fd] = (y - high.astype(jnp.float32)).astype(jnp.bfloat16)

    @pl.loop(1, n)
    def _(k):
        count_copy(k).wait_send()

    for t in range(3):
        own_pass(t, me).wait_send()
    guest_out.wait_send()
    share.wait_send()
    partial(0).wait_send()
    partial(1).wait_send()
    near.drain(early)
    full.drain(late)

    @pl.loop(0, side)
    def _(j):
        swap(j).wait_send()


def expert(pos, tokens, gate, up, down):
    n = lax.axis_size("wa")
    fd, hid = gate.shape
    half = fd // 2
    side = n // 2
    quarter = tokens.shape[1] // 4
    any_spec = pl.BlockSpec(memory_space=pl.ANY)
    vmem = pl.BlockSpec(memory_space=pltpu.VMEM)
    dma = pltpu.SemaphoreType.DMA
    return pl.pallas_call(
        functools.partial(expert_kernel, n),
        out_shape=jax.ShapeDtypeStruct((2 * CAP, side * fd), jnp.bfloat16),
        in_specs=[vmem, any_spec, any_spec, any_spec, any_spec],
        out_specs=vmem,
        scratch_shapes=[
            pltpu.VMEM((2, side, 2, half, hid), jnp.bfloat16),
            pltpu.VMEM((n, 2, half, hid), jnp.bfloat16),
            pltpu.VMEM((8, 128), jnp.int32),
            pltpu.VMEM((n, 8, 128), jnp.int32),
            pltpu.VMEM((3, CAP, quarter), jnp.bfloat16),
            pltpu.VMEM((2, CAP, quarter), jnp.bfloat16),
            pltpu.VMEM((2, tokens.shape[0], TOK_COLS), jnp.bfloat16),
            pltpu.VMEM((2, CAP, hid), jnp.bfloat16),
            pltpu.VMEM((2, CAP, hid), jnp.bfloat16),
            pltpu.VMEM((CAP, hid), jnp.float32),
            pltpu.VMEM((CAP, hid), jnp.float32),
            pltpu.VMEM((CAP, hid), jnp.bfloat16),
            pltpu.VMEM((side, CAP, fd), jnp.float32),
            pltpu.VMEM((side, CAP, fd), jnp.bfloat16),
            pltpu.VMEM((side, CAP, fd), jnp.bfloat16),
            dma((3,)), dma((2,)), dma((n,)), dma((n,)),
            *[dma((2, n // 8, 4)) for _ in range(4)],
            *[dma((2, n // 4, 2)) for _ in range(4)],
            dma((3,)), dma((3,)), dma, dma, dma, dma, dma((2,)), dma((2,)), dma((side,)), dma((side,)),
        ],
        compiler_params=pltpu.CompilerParams(
            collective_id=0, has_side_effects=True, vmem_limit_bytes=60 * 1024 * 1024
        ),
    )(pos, tokens, *(v.reshape(2, half, hid) for v in (gate, up, down)))


def per_device(tokens, expert_ids, keep_mask, route_weight, gate_weight, up_weight, down_weight):
    matches = (expert_ids == 0) & (keep_mask == 1)
    chosen = jnp.any(matches, axis=1).astype(jnp.int32)
    route_sum = jnp.sum(jnp.where(matches, route_weight, jnp.float32(0.0)), axis=1)
    position = jnp.cumsum(chosen) - chosen
    place = jnp.where(chosen == 1, position, -1)
    y = expert(place[None, :], tokens, gate_weight, up_weight, down_weight)
    slot_ids = lax.rem(jnp.arange(2 * CAP, dtype=jnp.int32), CAP)
    combine = (place[:, None] == slot_ids[None, :]).astype(jnp.bfloat16)
    mixed = jnp.dot(combine, y, preferred_element_type=jnp.float32)
    return (mixed * route_sum[:, None]).astype(jnp.bfloat16)


def solution(mesh):
    return jax.shard_map(
        per_device,
        mesh=mesh,
        in_specs=(
            P("wa", None),
            P("wa", None),
            P("wa", None),
            P("wa", None),
            P("wa", "ha"),
            P("wa", "ha"),
            P("wa", "ha"),
        ),
        out_specs=P("wa", "ha"),
        check_vma=False,
    )
```
